512 devices in a mesh: section: 16 (over x, y_lo), dp: 32 (over z, y_hi, core).
Axes of the slice: x: 4, y: 8 (y_hi: 2, y_lo: 4; y = y_hi * 4 + y_lo), z: 8, core: 2. Of those that a mesh axis runs over, the one named last changes fastest.
Arguments:
- acts: bfloat16 [16, 4, 1024, 4096], P('section', None, 'dp'), may hold values from -6 to 6
- grads_out: bfloat16 [16, 4, 1024, 4096], P('section', None, 'dp'), may hold values from -6 to 6
- weight_grad: bfloat16 [16, 4096, 4096], P('section', 'dp'), may hold values from -16 to 16
- old_in_factor: float32 [16, 32, 128, 128], P('section', 'dp'), may hold values from -12 to 24, as said below
- old_out_factor: float32 [16, 32, 128, 128], P('section', 'dp'), may hold values from -12 to 24, as said below
Outputs:
- update: bfloat16 [16, 4096, 4096], P('section', 'dp')
- in_factor: float32 [16, 32, 128, 128], P('section', 'dp')
- out_factor: float32 [16, 32, 128, 128], P('section', 'dp')
The draws below stay inside these ranges and needn't reach their ends.
Inputs may be any that keep to these rules, and one draw needn't show every extreme that they name: `old_in_factor`: each block is symmetric positive definite. `old_out_factor`: each block is symmetric positive definite.
All inputs are finite; a program needn't handle non-finite values.
Results may differ from the reference program's by a relative error of at most 0.0064.
Values may be sent and summed in bfloat16 or wider, within the bound.
A program may use at most 64 MiB of HBM per device.

```python
import jax
import jax.numpy as jnp
from jax import lax

D_IN = 4096
D_OUT = 4096
BLK = 128
MICRO = 4
ITERS = 8
TOKENS = 1024
LAYERS = 16
NBLK_IN = 32
NBLK_OUT = 32


def spd_blocks(key, count, shared):
    normal_key = jax.random.fold_in(jax.random.fold_in(key, 7), 0)
    level_key = jax.random.fold_in(jax.random.fold_in(key, 7), 2)
    rough = jax.random.normal(normal_key, (LAYERS, count, BLK, 2 * BLK), jnp.float32)
    blocks = jnp.einsum('lbik,lbjk->lbij', rough, rough, precision=lax.Precision.HIGHEST) / (2 * BLK)
    if shared:
        levels = jnp.exp(jax.random.uniform(level_key, (1, count, 1, 1), jnp.float32, -1.4, 1.4))
    else:
        levels = jnp.exp(jax.random.uniform(level_key, (LAYERS, count, 1, 1), jnp.float32, -1.4, 1.4))
    return jnp.clip(blocks * levels, -12.0, 24.0)


def draw_old_in_factor(key, part):
    return spd_blocks(jax.random.fold_in(key, 11), NBLK_IN, False)


def draw_old_out_factor(key, part):
    return spd_blocks(jax.random.fold_in(key, 13), NBLK_OUT, True)


def draw_weight_grad(key, part):
    main_key = jax.random.fold_in(jax.random.fold_in(key, 17), 0)
    level_key = jax.random.fold_in(jax.random.fold_in(key, 17), 2)
    widest = max(NBLK_IN, NBLK_OUT)
    levels = jnp.exp(jax.random.uniform(level_key, (LAYERS, widest), jnp.float32, -0.85, 0.85))
    row_scale = jnp.repeat(levels[:, :NBLK_OUT], BLK, axis=1)
    col_scale = jnp.repeat(levels[:, :NBLK_IN], BLK, axis=1)
    values = jax.random.normal(main_key, (LAYERS, D_OUT, D_IN), jnp.float32)
    scaled = values * row_scale[:, :, None] * col_scale[:, None, :]
    return jnp.clip(scaled, -16.0, 16.0).astype(jnp.bfloat16)


def block_levels(stream_key, dims, cuts, smallest, top_value):
    def one(axis_at, parts):
        draws = jax.random.uniform(jax.random.fold_in(jax.random.fold_in(stream_key, 6), axis_at), (parts,), jnp.float32, smallest / len(cuts), top_value / len(cuts))
        return jnp.repeat(jnp.exp(draws), dims[axis_at] // parts).reshape((-1,) + (1,) * (len(dims) - axis_at - 1))

    factor_of = one(*cuts[0])
    for cut in cuts[1:]:
        factor_of = factor_of * one(*cut)
    return factor_of


def centred(own_key, extent, spread, bound, cuts=(), kind=jnp.bfloat16):
    gain = block_levels(own_key, extent, cuts, -0.22, 0.18) if cuts else 1.0
    result = jax.random.normal(own_key, extent, jnp.float32) * spread * gain
    return jnp.minimum(jnp.maximum(result, -bound), bound).astype(kind)


def setup_inputs(seed: int = 0) -> dict:
    streams_of = jax.random.split(jax.random.key(seed), 6)
    return {
        "acts": centred(streams_of[0], (LAYERS, MICRO, TOKENS, D_IN), 1.0, 6.0, ((0, 16), (2, 32))),
        "grads_out": centred(streams_of[1], (LAYERS, MICRO, TOKENS, D_OUT), 1.0, 6.0, ((0, 16), (2, 32))),
        "weight_grad": draw_weight_grad(jax.random.fold_in(streams_of[5], 71), 0),
        "old_in_factor": draw_old_in_factor(jax.random.fold_in(streams_of[5], 71), 0),
        "old_out_factor": draw_old_out_factor(jax.random.fold_in(streams_of[5], 71), 0),
    }


DECAY = 0.7
DAMPING = 0.1
CLIP = 0.04
HIGH = lax.Precision.HIGHEST

def newton(factor):
    size = factor.shape[-1]
    eye = jnp.eye(size, dtype=jnp.float32)
    damped = factor + DAMPING * eye
    norms = jnp.sqrt(lax.optimization_barrier(jnp.sum(damped * damped, axis=(1, 2))))
    approx = eye[None] / norms[:, None, None]
    for sweep in range(ITERS):
        product = jnp.einsum('bij,bjk->bik', damped, approx, precision=HIGH)
        approx = jnp.einsum('bij,bjk->bik', approx, 2.0 * eye - product, precision=HIGH)
    return approx

def one_layer(items):
    acts_l, grads_l, wgrad_l, old_in, old_out = items
    count = MICRO * TOKENS
    flat_in = acts_l.reshape(-1, NBLK_IN, BLK).astype(jnp.float32)
    flat_out = grads_l.reshape(-1, NBLK_OUT, BLK).astype(jnp.float32)
    gram_in = jnp.einsum('tbi,tbj->bij', flat_in, flat_in, precision=HIGH) / count
    gram_out = jnp.einsum('tbi,tbj->bij', flat_out, flat_out, precision=HIGH) / count
    in_factor = DECAY * old_in + (1.0 - DECAY) * gram_in
    out_factor = DECAY * old_out + (1.0 - DECAY) * gram_out
    in_inverse = newton(in_factor).astype(jnp.bfloat16)
    out_inverse = newton(out_factor).astype(jnp.bfloat16)
    blocks = wgrad_l.reshape(NBLK_OUT, BLK, D_IN).astype(jnp.float32)
    left = jnp.einsum('bij,bjd->bid', out_inverse.astype(jnp.float32), blocks, precision=HIGH)
    left = left.astype(jnp.bfloat16).reshape(D_OUT, NBLK_IN, BLK)
    natural = jnp.einsum('rci,cij->rcj', left.astype(jnp.float32), in_inverse.astype(jnp.float32), precision=HIGH)
    natural = natural.reshape(D_OUT, D_IN)
    quad_part = jnp.sum(natural * wgrad_l.astype(jnp.float32))
    return (natural, quad_part, in_factor, out_factor)

def reference(acts, grads_out, weight_grad, old_in_factor, old_out_factor):
    natural, quad_parts, in_factor, out_factor = lax.map(one_layer, (acts, grads_out, weight_grad, old_in_factor, old_out_factor))
    quad = jnp.sum(quad_parts)
    numel = LAYERS * D_OUT * D_IN
    scale = jnp.minimum(1.0, jnp.sqrt(CLIP * numel / quad))
    update = (scale * natural).astype(jnp.bfloat16)
    return (update, in_factor, out_factor)
```

```python
import jax
import jax.numpy as jnp
from jax import lax
from jax.experimental import pallas as pl
from jax.experimental.pallas import tpu as pltpu
from jax.sharding import Mesh
from jax.sharding import PartitionSpec as P

ITERS = 8
SECTION = ("section_0", "section_1")
DP = ("dp_0", "dp_1", "dp_2")
DECAY = 0.7
DAMPING = 0.1
CLIP = 0.04
HIGH = lax.Precision.HIGHEST
MESH_ID = pl.DeviceIdType.MESH

X, YL, Z, YH, CORE = 4, 4, 8, 2, 2
CHIPS = Z * YH
B = 128
H = B // 2
ROWS = H + 8
F32 = jnp.float32
BF16 = jnp.bfloat16


def iotas():
    return (
        lax.broadcasted_iota(jnp.int32, (H, B), 0),
        lax.broadcasted_iota(jnp.int32, (H, B), 1),
    )


def pack(full):
    r, l = iotas()
    top, low = full[:H], pltpu.roll(full[H:], H, 1)
    body = jnp.where((l < H) & (r > l), low, top)
    diag = jnp.sum(jnp.where(r == l, low, 0.0), axis=0, keepdims=True)
    return body, jnp.broadcast_to(diag, (8, B))


def unpack(packed):
    r, l = iotas()
    body, diag = packed[:H], packed[H : H + 1]
    turned = jnp.concatenate([body, jnp.zeros((H, B), F32)], axis=0).T
    left_t, right_t = turned[:H], turned[H:]
    top = jnp.where((l < H) & (r > l), left_t, body)
    corner = jnp.where(r > l, body, jnp.where(r == l, diag, left_t))
    bottom = jnp.where(l < H, right_t, pltpu.roll(corner, H, 1))
    return jnp.concatenate([top, bottom], axis=0)


def eye():
    return (
        lax.broadcasted_iota(jnp.int32, (B, B), 0) == lax.broadcasted_iota(jnp.int32, (B, B), 1)
    ).astype(F32)


def dot(a, b):
    return jnp.dot(a, b, precision=HIGH, preferred_element_type=F32)


def newton(factor):
    one = eye()
    damped = factor + DAMPING * one
    inv = 1.0 / jnp.sqrt(jnp.sum(damped * damped, keepdims=True))
    rest = one - inv * damped
    approx = inv * (one + rest)
    rest = dot(rest, rest)
    for _ in range(ITERS - 2):
        both = dot(rest, jnp.concatenate([rest, approx], axis=1))
        approx = approx + both[:, B:]
        rest = both[:, :B]
    return approx + dot(rest, approx)


def offsets(i):
    j = i // 2
    dz = 4 + ((j + 1) // 2) * (1 - 2 * (j % 2))
    return dz, 1 - i % 2


def kernel(
    acts, grads, wgrad, old_in, old_out,
    nat_o, fin_o, fout_o, scale_o,
    tok_in, tok_out, wv, oi, oo, fi, fo,
    pk_in, pk_out, own_in, own_out, d2d_in, d2d_out,
    comb_in, comb_out, rx_in, rx_out,
    xall, left, nat, q1, q2, mine, mine2,
    ld, st, d_s, d_r, a_s, a_r, g_s, g_r, f_s, f_r, s1, r1, s2, r2,
):
    x, yl = lax.axis_index("section_0"), lax.axis_index("section_1")
    z, yh, c = lax.axis_index("dp_0"), lax.axis_index("dp_1"), lax.axis_index("dp_2")
    q_me = z * YH + yh
    other = {"dp_2": 1 - c}

    loads = [
        pltpu.make_async_copy(acts.at[0], tok_in, ld.at[0]),
        pltpu.make_async_copy(grads.at[0], tok_out, ld.at[1]),
        pltpu.make_async_copy(old_in.at[0, 0], oi, ld.at[2]),
        pltpu.make_async_copy(old_out.at[0, 0], oo, ld.at[3]),
        pltpu.make_async_copy(wgrad.at[0], wv, ld.at[4]),
    ]
    for copy in loads:
        copy.start()

    def chip_to(i):
        dz, dy = offsets(i)
        return (z + dz) % Z, (yh + dy) % YH

    def chip_from(i):
        dz, dy = offsets(i)
        return (z + Z - dz) % Z, (yh + dy) % YH

    def plane_to(k):
        y = (yh * YL + yl + k % 8) % 8
        return {"section_0": (x + k // 8) % X, "section_1": y % YL, "dp_1": y // YL}

    def column_to(k):
        return {"dp_0": (z + k // 2) % Z, "dp_2": (c + k % 2) % CORE}

    barrier = pltpu.get_barrier_semaphore()
    pl.semaphore_signal(barrier, inc=1, device_id=other, device_id_type=MESH_ID)

    @pl.loop(0, CHIPS - 1)
    def _(i):
        tz, ty = chip_to(i)
        pl.semaphore_signal(
            barrier, inc=1, device_id={"dp_0": tz, "dp_1": ty}, device_id_type=MESH_ID
        )

    @pl.loop(1, X * 8)
    def _(k):
        @pl.when(k != 4)
        def _():
            pl.semaphore_signal(barrier, inc=1, device_id=plane_to(k), device_id_type=MESH_ID)

    @pl.loop(1, Z)
    def _(k):
        pl.semaphore_signal(
            barrier, inc=1, device_id=column_to(2 * k + 1), device_id_type=MESH_ID
        )

    def gram(tok, p, core):
        at = pl.multiple_of((p * CORE + core) * B, B)
        t = tok[:, :, pl.ds(at, B)].reshape(B, B)
        return lax.dot_general(t, t, (((0,), (0,)), ((), ())), preferred_element_type=F32)

    def for_partner(tok, out):
        @pl.loop(0, CHIPS)
        def _(p):
            body, diag = pack(gram(tok, p, 1 - c))
            out[p, :H] = body.astype(BF16)
            out[p, H:] = diag.astype(BF16)

    def for_me(tok, out):
        @pl.loop(0, CHIPS)
        def _(p):
            body, diag = pack(gram(tok, p, c))
            out[p, :H] = body
            out[p, H:] = diag

    def to_partner(kind, src, dst):
        return pltpu.make_async_remote_copy(
            src_ref=src, dst_ref=dst, send_sem=d_s.at[kind], recv_sem=d_r.at[kind],
            device_id=other, device_id_type=MESH_ID,
        )

    def exchange(kind, src, dst, i, slot_from, slot_to, tz, ty):
        return pltpu.make_async_remote_copy(
            src_ref=src.at[slot_from], dst_ref=dst.at[slot_to],
            send_sem=a_s.at[kind, i], recv_sem=a_r.at[kind, slot_to],
            device_id={"dp_0": tz, "dp_1": ty}, device_id_type=MESH_ID,
        )

    def combine(kind, own, got, comb, rx):
        @pl.loop(0, CHIPS - 1)
        def _(i):
            tz, ty = chip_to(i)
            q = tz * YH + ty
            comb[q] = (own[q] + got[q].astype(F32)).astype(BF16)
            exchange(kind, comb, rx, i, q, q_me, tz, ty).start()

    def collect(kind, own, got, comb, rx):
        acc = own[q_me] + got[q_me].astype(F32)

        def step(i, acc):
            fz, fy = chip_from(CHIPS - 2 - i)
            q = fz * YH + fy
            exchange(kind, comb, rx, CHIPS - 2 - i, q, q, fz, fy).wait_recv()
            return acc + rx[q].astype(F32)

        return lax.fori_loop(0, CHIPS - 1, step, acc)

    count = F32(4.0 * 32 * Z * YH * CORE)

    loads[0].wait()
    for_partner(tok_in, pk_in)
    for_me(tok_in, own_in)
    pl.semaphore_wait(barrier, 1 + (CHIPS - 1) + (X * 8 - 2) + (Z - 1))
    in_pair = to_partner(0, pk_in, d2d_in)
    in_pair.start()
    loads[1].wait()
    for_partner(tok_out, pk_out)
    out_pair = to_partner(1, pk_out, d2d_out)
    out_pair.start()
    in_pair.wait_recv()
    combine(0, own_in, d2d_in, comb_in, rx_in)
    for_me(tok_out, own_out)
    out_pair.wait_recv()
    combine(1, own_out, d2d_out, comb_out, rx_out)
    for copy in loads[2:]:
        copy.wait()

    gram_in = unpack(collect(0, own_in, d2d_in, comb_in, rx_in))
    in_factor = DECAY * oi[...] + ((1.0 - DECAY) / count) * gram_in
    fi[...] = in_factor
    body, diag = pack(newton(in_factor))
    b_me = q_me * CORE + c
    xall[b_me, :H] = body.astype(BF16)
    xall[b_me, H:] = diag.astype(BF16)

    def gather(i, slot, q, tz, ty):
        return pltpu.make_async_remote_copy(
            src_ref=xall.at[slot], dst_ref=xall.at[slot],
            send_sem=g_s.at[i], recv_sem=g_r.at[q],
            device_id={"dp_0": tz, "dp_1": ty}, device_id_type=MESH_ID,
        )

    def forward(slot, q):
        return pltpu.make_async_remote_copy(
            src_ref=xall.at[slot], dst_ref=xall.at[slot],
            send_sem=f_s.at[q], recv_sem=f_r.at[q],
            device_id=other, device_id_type=MESH_ID,
        )

    forward(b_me, q_me).start()

    @pl.loop(0, CHIPS - 1)
    def _(i):
        tz, ty = chip_to(i)
        gather(i, b_me, q_me, tz, ty).start()

    save_in = pltpu.make_async_copy(fi, fin_o.at[0, 0], st.at[0])
    save_in.start()

    gram_out = unpack(collect(1, own_out, d2d_out, comb_out, rx_out))
    out_factor = DECAY * oo[...] + ((1.0 - DECAY) / count) * gram_out
    fo[...] = out_factor
    out_inverse = newton(out_factor).astype(BF16)
    save_out = pltpu.make_async_copy(fo, fout_o.at[0, 0], st.at[1])
    save_out.start()

    @pl.loop(0, 8)
    def _(k):
        at = pl.ds(pl.multiple_of(k * 512, 512), 512)
        left[:, at] = jnp.dot(out_inverse, wv[:, at], preferred_element_type=F32).astype(BF16)

    def block(slot, acc):
        inverse = unpack(xall[slot].astype(F32)).astype(BF16)
        at = pl.ds(pl.multiple_of(slot * B, B), B)
        part = jnp.dot(left[:, at], inverse, preferred_element_type=F32)
        nat[:, at] = part
        part = part * wv[:, at].astype(F32)
        return acc + jnp.sum(part.reshape(16, 8, B), axis=0)

    acc = block(b_me, jnp.zeros((8, B), F32))
    forward(b_me, q_me).wait_recv()
    acc = block(q_me * CORE + 1 - c, acc)

    def arrive(k, acc):
        i = CHIPS - 2 - k
        fz, fy = chip_from(i)
        q = fz * YH + fy
        slot = q * CORE + c
        gather(i, slot, q, fz, fy).wait_recv()
        forward(slot, q).start()
        acc = block(slot, acc)
        forward(slot, q).wait_recv()
        return block(q * CORE + 1 - c, acc)

    acc = lax.fori_loop(0, CHIPS - 1, arrive, acc)
    save_nat = pltpu.make_async_copy(nat, nat_o, st.at[2])
    save_nat.start()

    total = jnp.sum(acc)
    mine[...] = jnp.full((1, B), total, F32)

    def plane(k, slot):
        return pltpu.make_async_remote_copy(
            src_ref=mine, dst_ref=q1.at[slot], send_sem=s1.at[k], recv_sem=r1.at[slot],
            device_id=plane_to(k), device_id_type=MESH_ID,
        )

    def column(k, slot):
        return pltpu.make_async_remote_copy(
            src_ref=mine2, dst_ref=q2.at[slot], send_sem=s2.at[k], recv_sem=r2.at[slot],
            device_id=column_to(k), device_id_type=MESH_ID,
        )

    @pl.loop(1, X * 8)
    def _(k):
        plane(k, k).start()

    quad = mine[...]

    def plane_sum(k, quad):
        plane(k, k).wait_recv()
        return quad + q1[k]

    quad = lax.fori_loop(1, X * 8, plane_sum, quad)
    mine2[...] = quad

    @pl.loop(1, Z * CORE)
    def _(k):
        column(k, k).start()

    def column_sum(k, quad):
        column(k, k).wait_recv()
        return quad + q2[k]

    quad = lax.fori_loop(1, Z * CORE, column_sum, quad)
    numel = F32(X * YL * 4096.0 * 4096.0)
    scale_o[...] = jnp.minimum(1.0, jnp.sqrt(CLIP * numel / quad))

    in_pair.wait_send()
    out_pair.wait_send()
    forward(b_me, q_me).wait_send()

    @pl.loop(0, CHIPS - 1)
    def _(i):
        tz, ty = chip_to(i)
        exchange(0, comb_in, rx_in, i, 0, 0, tz, ty).wait_send()
        exchange(1, comb_out, rx_out, i, 0, 0, tz, ty).wait_send()
        gather(i, b_me, q_me, tz, ty).wait_send()
        q = tz * YH + ty
        forward(q * CORE + c, q).wait_send()

    @pl.loop(1, X * 8)
    def _(k):
        plane(k, k).wait_send()

    @pl.loop(1, Z * CORE)
    def _(k):
        column(k, k).wait_send()

    save_in.wait()
    save_out.wait()
    save_nat.wait()


def body(acts, grads_out, weight_grad, old_in_factor, old_out_factor):
    rows, width = weight_grad.shape[1:]
    any_space = pl.BlockSpec(memory_space=pl.ANY)
    dma = pltpu.SemaphoreType.DMA
    vmem = pltpu.VMEM
    packed = (CHIPS, ROWS, B)
    nat, in_factor, out_factor, scale = pl.pallas_call(
        kernel,
        out_shape=(
            jax.ShapeDtypeStruct((rows, width), F32),
            jax.ShapeDtypeStruct(old_in_factor.shape, F32),
            jax.ShapeDtypeStruct(old_out_factor.shape, F32),
            jax.ShapeDtypeStruct((1, B), F32),
        ),
        in_specs=[any_space] * 5,
        out_specs=(any_space, any_space, any_space, pl.BlockSpec(memory_space=vmem)),
        scratch_shapes=[
            vmem(acts.shape[1:], BF16),
            vmem(acts.shape[1:], BF16),
            vmem((rows, width), BF16),
            vmem((B, B), F32),
            vmem((B, B), F32),
            vmem((B, B), F32),
            vmem((B, B), F32),
            vmem(packed, BF16),
            vmem(packed, BF16),
            vmem(packed, F32),
            vmem(packed, F32),
            vmem(packed, BF16),
            vmem(packed, BF16),
            vmem(packed, BF16),
            vmem(packed, BF16),
            vmem(packed, BF16),
            vmem(packed, BF16),
            vmem((CHIPS * CORE, ROWS, B), BF16),
            vmem((rows, width), BF16),
            vmem((rows, width), F32),
            vmem((X * 8, 1, B), F32),
            vmem((Z * CORE, 1, B), F32),
            vmem((1, B), F32),
            vmem((1, B), F32),
            dma((5,)),
            dma((3,)),
            dma((2,)),
            dma((2,)),
            dma((2, CHIPS)),
            dma((2, CHIPS)),
            dma((CHIPS,)),
            dma((CHIPS,)),
            dma((CHIPS,)),
            dma((CHIPS,)),
            dma((X * 8,)),
            dma((X * 8,)),
            dma((Z * CORE,)),
            dma((Z * CORE,)),
        ],
        compiler_params=pltpu.CompilerParams(
            collective_id=1, has_side_effects=True, vmem_limit_bytes=60 * 1024 * 1024
        ),
        name="kfac",
    )(acts, grads_out, weight_grad, old_in_factor, old_out_factor)
    update = (scale[0, 0] * nat).astype(BF16)
    return (update[None], in_factor, out_factor)


def solution(mesh):
    torus = Mesh(
        mesh.devices.reshape(X, YL, Z, YH, CORE),
        ("section_0", "section_1", "dp_0", "dp_1", "dp_2"),
    )
    in_specs = (
        P(SECTION, None, DP, None),
        P(SECTION, None, DP, None),
        P(SECTION, DP, None),
        P(SECTION, DP, None, None),
        P(SECTION, DP, None, None),
    )
    out_specs = (P(SECTION, DP, None), P(SECTION, DP, None, None), P(SECTION, DP, None, None))
    return jax.shard_map(body, mesh=torus, in_specs=in_specs, out_specs=out_specs, check_vma=False)
```

```python
import jax
import jax.numpy as jnp
from jax import lax
from jax.experimental import pallas as pl
from jax.experimental.pallas import tpu as pltpu
from jax.sharding import Mesh
from jax.sharding import PartitionSpec as P

ITERS = 8
SECTION = ("section_0", "section_1")
DP = ("dp_0", "dp_1", "dp_2")
DECAY = 0.7
DAMPING = 0.1
CLIP = 0.04
HIGH = lax.Precision.HIGHEST
LOGICAL = pl.DeviceIdType.LOGICAL

X, YL, Z, YH, CORE = 4, 4, 8, 2, 2
Y = YH * YL
CHIPS = Z * YH
PEERS = CHIPS - 1
B = 128
H = B // 2
ROWS = H + 8
GROUP = 3
F32 = jnp.float32
BF16 = jnp.bfloat16


def iotas():
    return (
        lax.broadcasted_iota(jnp.int32, (H, B), 0),
        lax.broadcasted_iota(jnp.int32, (H, B), 1),
    )


def pack(full):
    r, l = iotas()
    top, low = full[:H], pltpu.roll(full[H:], H, 1)
    body = jnp.where((l < H) & (r > l), low, top)
    diag = jnp.sum(jnp.where(r == l, low, 0.0).reshape(H // 8, 8, B), axis=0)
    return body, diag


def unpack(packed):
    r, l = iotas()
    body, diag = packed[:H], packed[H:]
    turned = jnp.concatenate([body, jnp.zeros((H, B), F32)], axis=0).T
    left_t, right_t = turned[:H], turned[H:]
    top = jnp.where((l < H) & (r > l), left_t, body)
    spread = jnp.concatenate([diag] * (H // 8), axis=0)
    corner = jnp.where(r > l, body, jnp.where(r == l, spread, left_t))
    bottom = jnp.where(l < H, right_t, pltpu.roll(corner, H, 1))
    return jnp.concatenate([top, bottom], axis=0)


def eye():
    return (
        lax.broadcasted_iota(jnp.int32, (B, B), 0) == lax.broadcasted_iota(jnp.int32, (B, B), 1)
    ).astype(F32)


def dot(a, b):
    return jnp.dot(a, b, precision=HIGH, preferred_element_type=F32)


def newton(factor):
    one = eye()
    damped = factor + DAMPING * one
    inv = 1.0 / jnp.sqrt(jnp.sum(damped * damped, keepdims=True))
    rest = one - inv * damped
    approx = inv * (one + rest)
    rest = dot(rest, rest)
    for _ in range(ITERS - 2):
        both = dot(rest, jnp.concatenate([rest, approx], axis=1))
        approx = approx + both[:, B:]
        rest = both[:, :B]
    return approx + dot(rest, approx)


def offset(i):
    j = i // 2
    return 4 + ((j + 1) // 2) * (1 - 2 * (j % 2)), 1 - i % 2


def kernel(
    acts, grads, wgrad, old_in, old_out,
    nat, fi, fo, scale_o,
    tok_in, tok_out, wv, oi, oo,
    pk_in, pk_out, own_in, own_out, d2d_in, d2d_out,
    comb_in, comb_out, rx_in, rx_out,
    xd, xf, left, q1, q2, mine, mine2,
    ld, d_s, d_r, a_s, a_r, g_s, g_r, f_s, f_r, q_s, q_r,
):
    x, yl = lax.axis_index("section_0"), lax.axis_index("section_1")
    z, yh, c = lax.axis_index("dp_0"), lax.axis_index("dp_1"), lax.axis_index("dp_2")
    y = yh * YL + yl

    loads = [
        pltpu.make_async_copy(acts.at[0], tok_in, ld.at[0]),
        pltpu.make_async_copy(grads.at[0], tok_out, ld.at[1]),
        pltpu.make_async_copy(old_in.at[0, 0], oi, ld.at[2]),
        pltpu.make_async_copy(old_out.at[0, 0], oo, ld.at[3]),
        pltpu.make_async_copy(wgrad.at[0], wv, ld.at[4]),
    ]
    for copy in loads:
        copy.start()

    z_ahead = [lax.rem(z + d, Z) for d in range(Z)]
    y_ahead = [lax.rem(y + d, Y) for d in range(Y)]
    x_at = [lax.rem(x + d, X) * (YL * Z * YH * CORE) for d in range(X)]
    y_at = [lax.rem(t, YL) * (Z * YH * CORE) + lax.div(t, YL) * CORE for t in y_ahead]
    z_at = [t * (YH * CORE) for t in z_ahead]
    c_at = [c, 1 - c]

    def device(dx=0, dy=0, dz=0, dc=0):
        return x_at[dx] + y_at[dy] + z_at[dz] + c_at[dc]

    partner = device(dc=1)
    chips = [device(dy=YL * offset(i)[1], dz=offset(i)[0]) for i in range(PEERS)]
    plane = [(dx, dy) for dx in (2, 1, 3, 0) for dy in (4, 3, 5, 2, 6, 1, 7, 0)][:-1]
    column = [(dz, dc) for dz in (4, 3, 5, 2, 6, 1, 7, 0) for dc in (1, 0)][:-1]
    planes = [device(dx=dx, dy=dy) for dx, dy in plane]
    columns = [device(dz=dz, dc=dc) for dz, dc in column]
    greeted = (
        [partner]
        + chips
        + [d for d, at in zip(planes, plane, strict=True) if at != (0, YL)]
        + [d for d, at in zip(columns, column, strict=True) if at[0] and at[1]]
    )
    barrier = pltpu.get_barrier_semaphore()
    for target in greeted:
        pl.semaphore_signal(barrier, inc=1, device_id=target, device_id_type=LOGICAL)

    def chip_to(i):
        dz, dy = offset(i)
        return lax.rem(z + dz, Z) * YH + lax.rem(yh + dy, YH)

    def chip_from(i):
        dz, dy = offset(i)
        return lax.rem(z + Z - dz, Z) * YH + lax.rem(yh + dy, YH)

    def columns_of(chip, core):
        return pl.ds(pl.multiple_of((chip * CORE + core) * B, B), B)

    def grams(tok, core, out):
        @pl.loop(0, CHIPS // 4)
        def _(g):
            for u in range(4):
                i = g * 4 + u
                t = tok[:, :, columns_of(chip_to(i), core)].reshape(B, B)
                full = lax.dot_general(
                    t, t, (((0,), (0,)), ((), ())), preferred_element_type=F32
                )
                body, diag = pack(full)
                out[i, :H] = body.astype(out.dtype)
                out[i, H:] = diag.astype(out.dtype)

    def remote(src, dst, send, recv, target):
        return pltpu.make_async_remote_copy(
            src_ref=src, dst_ref=dst, send_sem=send, recv_sem=recv,
            device_id=target, device_id_type=LOGICAL,
        )

    def combine(kind, own, got, comb, rx):
        for i in range(PEERS):
            comb[i] = (own[i] + got[i].astype(F32)).astype(BF16)
            remote(comb.at[i], rx.at[i], a_s.at[kind], a_r.at[kind], chips[i]).start()

    def whole(ref, sem):
        return pltpu.make_async_copy(ref, ref, sem)

    def collect(kind, own, got, rx):
        acc = own[PEERS] + got[PEERS].astype(F32)
        whole(rx, a_r.at[kind]).wait()
        for i in range(PEERS):
            acc = acc + rx[i].astype(F32)
        return acc

    count = F32(4.0 * 32 * Z * YH * CORE)

    loads[0].wait()
    grams(tok_in, 1 - c, pk_in)
    pl.semaphore_wait(barrier, len(greeted))
    in_pair = remote(pk_in, d2d_in, d_s.at[0], d_r.at[0], partner)
    in_pair.start()
    grams(tok_in, c, own_in)
    in_pair.wait_recv()
    combine(0, own_in, d2d_in, comb_in, rx_in)
    loads[1].wait()
    grams(tok_out, 1 - c, pk_out)
    out_pair = remote(pk_out, d2d_out, d_s.at[1], d_r.at[1], partner)
    out_pair.start()
    grams(tok_out, c, own_out)
    out_pair.wait_recv()
    combine(1, own_out, d2d_out, comb_out, rx_out)
    for copy in loads[2:]:
        copy.wait()

    gram_in = unpack(collect(0, own_in, d2d_in, rx_in))
    in_factor = DECAY * oi[...] + ((1.0 - DECAY) / count) * gram_in
    fi[...] = in_factor
    body, diag = pack(newton(in_factor))
    xd[PEERS, :H] = body.astype(BF16)
    xd[PEERS, H:] = diag.astype(BF16)

    def gather(i):
        return remote(xd.at[PEERS], xd.at[i], g_s, g_r.at[i], partner)

    def forward(i):
        return remote(xd.at[i], xf.at[i], f_s, f_r.at[i], partner)

    for i in range(PEERS):
        remote(xd.at[PEERS], xd.at[i], g_s, g_r.at[i], chips[i]).start()
    forward(PEERS).start()

    gram_out = unpack(collect(1, own_out, d2d_out, rx_out))
    out_factor = DECAY * oo[...] + ((1.0 - DECAY) / count) * gram_out
    fo[...] = out_factor
    out_inverse = newton(out_factor).astype(BF16)

    @pl.loop(0, 2)
    def _(k):
        for u in range(4):
            at = pl.ds(pl.multiple_of(k * 2048 + u * 512, 512), 512)
            left[:, at] = jnp.dot(out_inverse, wv[:, at], preferred_element_type=F32).astype(BF16)

    def block(packed, i, core, acc):
        inverse = unpack(packed[i].astype(F32)).astype(BF16)
        at = columns_of(chip_from(i), core)
        part = jnp.dot(left[:, at], inverse, preferred_element_type=F32)
        nat[:, at] = part
        part = part * wv[:, at].astype(F32)
        return acc + jnp.sum(part.reshape(B // 8, 8, B), axis=0)

    def arrivals(g):
        these = [PEERS - 1 - g * GROUP - u for u in range(GROUP)]
        for i in these:
            gather(i).wait_recv()
            forward(i).start()
        return these

    acc = block(xd, PEERS, c, jnp.zeros((8, B), F32))
    forward(PEERS).wait_recv()
    acc = block(xf, PEERS, 1 - c, acc)
    for i in arrivals(0):
        acc = block(xd, i, c, acc)

    def arrive(g, acc):
        these = arrivals(g)
        for i in these:
            forward(i + GROUP).wait_recv()
        for i in these:
            acc = block(xd, i, c, acc)
            acc = block(xf, i + GROUP, 1 - c, acc)
        return acc

    acc = lax.fori_loop(1, PEERS // GROUP, arrive, acc)
    for i in range(GROUP):
        forward(i).wait_recv()
    for i in range(GROUP):
        acc = block(xf, i, 1 - c, acc)

    mine[...] = jnp.full((1, B), jnp.sum(acc), F32)
    for k, target in enumerate(planes):
        remote(mine, q1.at[k], q_s.at[0], q_r.at[0], target).start()
    whole(q1, q_r.at[0]).wait()
    quad = mine[...] + jnp.sum(q1[...], axis=0)
    mine2[...] = quad
    for k, target in enumerate(columns):
        remote(mine2, q2.at[k], q_s.at[1], q_r.at[1], target).start()
    whole(q2, q_r.at[1]).wait()
    quad = quad + jnp.sum(q2[...], axis=0)
    numel = F32(X * YL * 4096.0 * 4096.0)
    scale_o[...] = jnp.minimum(1.0, jnp.sqrt(CLIP * numel / quad))

    in_pair.wait_send()
    out_pair.wait_send()
    whole(comb_in, a_s.at[0]).wait()
    whole(comb_out, a_s.at[1]).wait()
    whole(rx_in, g_s).wait()
    whole(xf, f_s).wait()
    whole(q1, q_s.at[0]).wait()
    whole(q2, q_s.at[1]).wait()


def finish(nat, scale, in_factor, out_factor, update_o, in_o, out_o, up, sem):
    copies = [
        pltpu.make_async_copy(in_factor, in_o.at[0, 0], sem.at[0]),
        pltpu.make_async_copy(out_factor, out_o.at[0, 0], sem.at[1]),
    ]
    for copy in copies:
        copy.start()
    factor = scale[...]
    pieces, rows = 4, nat.shape[0] // 4
    for k in range(pieces):
        part = pl.ds(k * rows, rows)
        up[part] = (factor[:, :1] * nat[part]).astype(BF16)
        copy = pltpu.make_async_copy(up.at[part], update_o.at[0, part], sem.at[2 + k])
        copy.start()
        copies.append(copy)
    for copy in copies:
        copy.wait()


def body(acts, grads_out, weight_grad, old_in_factor, old_out_factor):
    rows, width = weight_grad.shape[1:]
    hbm = pl.BlockSpec(memory_space=pltpu.HBM)
    vm = pl.BlockSpec(memory_space=pltpu.VMEM)
    dma = pltpu.SemaphoreType.DMA
    vmem = pltpu.VMEM
    packed = (CHIPS, ROWS, B)
    sent = (PEERS, ROWS, B)
    operands = [
        pltpu.with_memory_space_constraint(a, pltpu.HBM)
        for a in (acts, grads_out, weight_grad, old_in_factor, old_out_factor)
    ]
    nat, in_factor, out_factor, scale = pl.pallas_call(
        kernel,
        out_shape=(
            jax.ShapeDtypeStruct((rows, width), F32),
            jax.ShapeDtypeStruct((B, B), F32),
            jax.ShapeDtypeStruct((B, B), F32),
            jax.ShapeDtypeStruct((1, B), F32),
        ),
        in_specs=[hbm] * 5,
        out_specs=(vm,) * 4,
        scratch_shapes=[
            vmem(acts.shape[1:], BF16),
            vmem(acts.shape[1:], BF16),
            vmem((rows, width), BF16),
            vmem((B, B), F32),
            vmem((B, B), F32),
            vmem(packed, BF16),
            vmem(packed, BF16),
            vmem(packed, F32),
            vmem(packed, F32),
            vmem(packed, BF16),
            vmem(packed, BF16),
            vmem(sent, BF16),
            vmem(sent, BF16),
            vmem(sent, BF16),
            vmem(sent, BF16),
            vmem(packed, BF16),
            vmem(packed, BF16),
            vmem((rows, width), BF16),
            vmem((X * Y - 1, 1, B), F32),
            vmem((Z * CORE - 1, 1, B), F32),
            vmem((1, B), F32),
            vmem((1, B), F32),
            dma((5,)),
            dma((2,)),
            dma((2,)),
            dma((2,)),
            dma((2,)),
            dma,
            dma((PEERS,)),
            dma,
            dma((CHIPS,)),
            dma((2,)),
            dma((2,)),
        ],
        compiler_params=pltpu.CompilerParams(
            collective_id=1, has_side_effects=True, vmem_limit_bytes=24 * 1024 * 1024
        ),
        name="kfac",
    )(*operands)
    return pl.pallas_call(
        finish,
        out_shape=(
            jax.ShapeDtypeStruct((1, rows, width), BF16),
            jax.ShapeDtypeStruct(old_in_factor.shape, F32),
            jax.ShapeDtypeStruct(old_out_factor.shape, F32),
        ),
        in_specs=[vm] * 4,
        out_specs=(hbm,) * 3,
        scratch_shapes=[vmem((rows, width), BF16), dma((6,))],
        compiler_params=pltpu.CompilerParams(vmem_limit_bytes=8 * 1024 * 1024),
        name="finish",
    )(nat, scale, in_factor, out_factor)


def solution(mesh):
    torus = Mesh(
        mesh.devices.reshape(X, YL, Z, YH, CORE),
        ("section_0", "section_1", "dp_0", "dp_1", "dp_2"),
    )
    in_specs = (
        P(SECTION, None, DP, None),
        P(SECTION, None, DP, None),
        P(SECTION, DP, None),
        P(SECTION, DP, None, None),
        P(SECTION, DP, None, None),
    )
    out_specs = (P(SECTION, DP, None), P(SECTION, DP, None, None), P(SECTION, DP, None, None))
    return jax.shard_map(body, mesh=torus, in_specs=in_specs, out_specs=out_specs, check_vma=False)
```

```python
import jax
import jax.numpy as jnp
from jax import lax
from jax.experimental import pallas as pl
from jax.experimental.pallas import tpu as pltpu
from jax.sharding import Mesh
from jax.sharding import PartitionSpec as P

ITERS = 8
SECTION = ("section_0", "section_1")
DP = ("dp_0", "dp_1", "dp_2")
DECAY = 0.7
DAMPING = 0.1
CLIP = 0.04
HIGH = lax.Precision.HIGHEST
LOGICAL = pl.DeviceIdType.LOGICAL

X, YL, Z, YH, CORE = 4, 4, 8, 2, 2
Y = YH * YL
CHIPS = Z * YH
PEERS = CHIPS - 1
B = 128
H = B // 2
ROWS = H + 8
SENT = H + 2
GROUP = 5
F32 = jnp.float32
BF16 = jnp.bfloat16


def iotas():
    return (
        lax.broadcasted_iota(jnp.int32, (H, B), 0),
        lax.broadcasted_iota(jnp.int32, (H, B), 1),
    )


def pack(full):
    r, l = iotas()
    top, low = full[:H], pltpu.roll(full[H:], H, 1)
    body = jnp.where((l < H) & (r > l), low, top)
    diag = jnp.sum(jnp.where(r == l, low, 0.0), axis=0, keepdims=True)
    return body, jnp.broadcast_to(diag, (ROWS - H, B))


def unpack(packed):
    r, l = iotas()
    body, diag = packed[:H], packed[H : H + 1]
    turned = jnp.concatenate([body, jnp.zeros((H, B), F32)], axis=0).T
    left_t, right_t = turned[:H], turned[H:]
    top = jnp.where((l < H) & (r > l), left_t, body)
    corner = jnp.where(r > l, body, jnp.where(r == l, diag, left_t))
    bottom = jnp.where(l < H, right_t, pltpu.roll(corner, H, 1))
    return jnp.concatenate([top, bottom], axis=0)


def eye():
    return (
        lax.broadcasted_iota(jnp.int32, (B, B), 0) == lax.broadcasted_iota(jnp.int32, (B, B), 1)
    ).astype(F32)


def parts(a):
    high = a.astype(BF16)
    return high, (a - high.astype(F32)).astype(BF16)


def dot(a, b):
    (ah, al), (bh, bl) = parts(a), parts(b)
    left = jnp.concatenate([ah, ah, al], axis=1)
    right = jnp.concatenate([bh, bl, bh], axis=0)
    return jnp.dot(left, right, preferred_element_type=F32)


def newton(factor):
    one = eye()
    damped = factor + DAMPING * one
    inv = 1.0 / jnp.sqrt(jnp.sum(damped * damped, keepdims=True))
    rest = one - inv * damped
    approx = inv * (one + rest)
    rest = dot(rest, rest)
    for _ in range(ITERS - 2):
        both = dot(rest, jnp.concatenate([rest, approx], axis=1))
        approx = approx + both[:, B:]
        rest = both[:, :B]
    return approx + dot(rest, approx)


def offset(i):
    j = i % Z
    return 4 + ((j + 1) // 2) * (1 - 2 * (j % 2)), 1 - i // Z


def kernel(
    acts, grads, wgrad, old_in, old_out,
    nat, fi, fo, scale_o,
    tok_in, tok_out, wv, oi, oo,
    pk_in, pk_out, own_in, own_out, d2d_in, d2d_out,
    comb_in, comb_out, rx_in, rx_out,
    xd, xf, left, q1, q2, mine, mine2,
    ld, d_s, d_r, a_s, a_r, g_s, g_r, f_s, f_r, q_s, q_r,
):
    x, yl = lax.axis_index("section_0"), lax.axis_index("section_1")
    z, yh, c = lax.axis_index("dp_0"), lax.axis_index("dp_1"), lax.axis_index("dp_2")
    y = yh * YL + yl

    loads = [
        pltpu.make_async_copy(acts.at[0], tok_in, ld.at[0]),
        pltpu.make_async_copy(grads.at[0], tok_out, ld.at[1]),
        pltpu.make_async_copy(old_in.at[0, 0], oi, ld.at[2]),
        pltpu.make_async_copy(old_out.at[0, 0], oo, ld.at[3]),
        pltpu.make_async_copy(wgrad.at[0], wv, ld.at[4]),
    ]
    for copy in loads:
        copy.start()

    z_ahead = [lax.rem(z + d, Z) for d in range(Z)]
    y_ahead = [lax.rem(y + d, Y) for d in range(Y)]
    x_at = [lax.rem(x + d, X) * (YL * Z * YH * CORE) for d in range(X)]
    y_at = [lax.rem(t, YL) * (Z * YH * CORE) + lax.div(t, YL) * CORE for t in y_ahead]
    z_at = [t * (YH * CORE) for t in z_ahead]
    c_at = [c, 1 - c]

    def device(dx=0, dy=0, dz=0, dc=0):
        return x_at[dx] + y_at[dy] + z_at[dz] + c_at[dc]

    partner = device(dc=1)
    chips = [device(dy=YL * offset(i)[1], dz=offset(i)[0]) for i in range(PEERS)]
    plane = [(dx, dy) for dx in (2, 1, 3, 0) for dy in (4, 3, 5, 2, 6, 1, 7, 0)][:-1]
    column = [(dz, dc) for dz in (4, 3, 5, 2, 6, 1, 7, 0) for dc in (1, 0)][:-1]
    planes = [device(dx=dx, dy=dy) for dx, dy in plane]
    columns = [device(dz=dz, dc=dc) for dz, dc in column]
    greeted = (
        [partner]
        + chips
        + [d for d, at in zip(planes, plane, strict=True) if at != (0, YL)]
        + [d for d, at in zip(columns, column, strict=True) if at[0] and at[1]]
    )
    barrier = pltpu.get_barrier_semaphore()
    for target in greeted:
        pl.semaphore_signal(barrier, inc=1, device_id=target, device_id_type=LOGICAL)

    def chip_to(i):
        dz, dy = offset(i)
        return lax.rem(z + dz, Z) * YH + lax.rem(yh + dy, YH)

    def chip_from(i):
        dz, dy = offset(i)
        return lax.rem(z + Z - dz, Z) * YH + lax.rem(yh + dy, YH)

    def columns_of(chip, core):
        return pl.ds(pl.multiple_of((chip * CORE + core) * B, B), B)

    def grams(tok, core, out):
        @pl.loop(0, CHIPS // 4)
        def _(g):
            for u in range(4):
                i = g * 4 + u
                t = tok[:, :, columns_of(chip_to(i), core)].reshape(B, B)
                full = lax.dot_general(
                    t, t, (((0,), (0,)), ((), ())), preferred_element_type=F32
                )
                body, diag = pack(full)
                out[i, :H] = body.astype(out.dtype)
                out[i, H:] = diag.astype(out.dtype)

    def remote(src, dst, send, recv, target):
        return pltpu.make_async_remote_copy(
            src_ref=src, dst_ref=dst, send_sem=send, recv_sem=recv,
            device_id=target, device_id_type=LOGICAL,
        )

    def sent(ref, at):
        return ref.at[at, pl.ds(0, SENT)]

    def combine(kind, own, got, comb, rx, these):
        for i in these:
            comb[i] = (own[i] + got[i].astype(F32)).astype(BF16)
            landed = a_r.at[kind, i // Z]
            remote(sent(comb, i), sent(rx, i), a_s.at[kind], landed, chips[i]).start()

    def whole(ref, sem):
        return pltpu.make_async_copy(ref, ref, sem)

    def collect(kind, side, rx, acc):
        these = (range(Z), range(Z, PEERS))[side]
        whole(sent(rx, pl.ds(these[0], len(these))), a_r.at[kind, side]).wait()
        for i in these:
            acc = acc + rx[i].astype(F32)
        return acc

    def mine_of(own, got):
        return own[PEERS] + got[PEERS].astype(F32)

    def halves(kind, src, dst):
        return [
            remote(sent(src, half), sent(dst, half), d_s.at[kind, h], d_r.at[kind, h], partner)
            for h, half in enumerate((pl.ds(0, Z), pl.ds(Z, Z)))
        ]

    count = F32(4.0 * 32 * Z * YH * CORE)

    loads[0].wait()
    grams(tok_in, 1 - c, pk_in)
    grams(tok_in, c, own_in)
    pl.semaphore_wait(barrier, len(greeted))
    in_pair = halves(0, pk_in, d2d_in)
    for half in in_pair:
        half.start()
    loads[1].wait()
    grams(tok_out, 1 - c, pk_out)
    out_pair = halves(1, pk_out, d2d_out)
    for half in out_pair:
        half.start()
    in_pair[0].wait_recv()
    combine(0, own_in, d2d_in, comb_in, rx_in, range(Z))
    in_pair[1].wait_recv()
    combine(0, own_in, d2d_in, comb_in, rx_in, range(Z, PEERS))
    grams(tok_out, c, own_out)
    for half in out_pair:
        half.wait_recv()
    for copy in loads[2:]:
        copy.wait()
    combine(1, own_out, d2d_out, comb_out, rx_out, range(PEERS))
    in_sum = collect(0, 1, rx_in, mine_of(own_in, d2d_in))
    gram_in = unpack(collect(0, 0, rx_in, in_sum))
    in_factor = DECAY * oi[...] + ((1.0 - DECAY) / count) * gram_in
    fi[...] = in_factor
    body, diag = pack(newton(in_factor))
    xd[PEERS, :H] = body.astype(BF16)
    xd[PEERS, H:] = diag.astype(BF16)

    def gather(i):
        return remote(sent(xd, PEERS), sent(xd, i), g_s, g_r.at[i], partner)

    def forward(i):
        return remote(sent(xd, i), sent(xf, i), f_s, f_r.at[i], partner)

    for i in range(PEERS):
        remote(sent(xd, PEERS), sent(xd, i), g_s, g_r.at[i], chips[i]).start()
    forward(PEERS).start()

    out_sum = collect(1, 1, rx_out, mine_of(own_out, d2d_out))
    gram_out = unpack(collect(1, 0, rx_out, out_sum))
    out_factor = DECAY * oo[...] + ((1.0 - DECAY) / count) * gram_out
    fo[...] = out_factor
    out_inverse = newton(out_factor).astype(BF16)

    @pl.loop(0, 2)
    def _(k):
        for u in range(4):
            at = pl.ds(pl.multiple_of(k * 2048 + u * 512, 512), 512)
            left[:, at] = jnp.dot(out_inverse, wv[:, at], preferred_element_type=F32).astype(BF16)

    def block(packed, i, core, acc):
        inverse = unpack(packed[i].astype(F32)).astype(BF16)
        at = columns_of(chip_from(i), core)
        part = jnp.dot(left[:, at], inverse, preferred_element_type=F32)
        nat[:, at] = part
        part = part * wv[:, at].astype(F32)
        return acc + jnp.sum(part.reshape(B // 8, 8, B), axis=0)

    def direct(g, acc):
        these = [PEERS - 1 - g * GROUP - u for u in range(GROUP)]
        for i in these:
            gather(i).wait_recv()
            forward(i).start()
        for i in these:
            acc = block(xd, i, c, acc)
        return acc

    def forwarded(g, acc):
        these = [PEERS - g * 4 - u for u in range(4)]
        for i in these:
            forward(i).wait_recv()
        for i in these:
            acc = block(xf, i, 1 - c, acc)
        return acc

    acc = block(xd, PEERS, c, jnp.zeros((8, B), F32))
    acc = lax.fori_loop(0, PEERS // GROUP, direct, acc)
    acc = lax.fori_loop(0, CHIPS // 4, forwarded, acc)

    mine[...] = jnp.full((1, B), jnp.sum(acc), F32)
    for k, target in enumerate(planes):
        remote(mine, q1.at[k], q_s.at[0], q_r.at[0], target).start()
    whole(q1, q_r.at[0]).wait()
    quad = mine[...] + jnp.sum(q1[...], axis=0)
    mine2[...] = quad
    for k, target in enumerate(columns):
        remote(mine2, q2.at[k], q_s.at[1], q_r.at[1], target).start()
    whole(q2, q_r.at[1]).wait()
    quad = quad + jnp.sum(q2[...], axis=0)
    numel = F32(X * YL * 4096.0 * 4096.0)
    scale_o[...] = jnp.minimum(1.0, jnp.sqrt(CLIP * numel / quad))

    for half in in_pair + out_pair:
        half.wait_send()
    every = pl.ds(0, PEERS)
    whole(sent(comb_in, every), a_s.at[0]).wait()
    whole(sent(comb_out, every), a_s.at[1]).wait()
    whole(sent(rx_in, every), g_s).wait()
    whole(sent(xf, pl.ds(0, CHIPS)), f_s).wait()
    whole(q1, q_s.at[0]).wait()
    whole(q2, q_s.at[1]).wait()


def finish(nat, scale, in_factor, out_factor, update_o, in_o, out_o, up, sem):
    copies = [
        pltpu.make_async_copy(in_factor, in_o.at[0, 0], sem.at[0]),
        pltpu.make_async_copy(out_factor, out_o.at[0, 0], sem.at[1]),
    ]
    for copy in copies:
        copy.start()
    factor = scale[...]
    pieces, rows = 4, nat.shape[0] // 4
    for k in range(pieces):
        part = pl.ds(k * rows, rows)
        up[part] = (factor[:, :1] * nat[part]).astype(BF16)
        copy = pltpu.make_async_copy(up.at[part], update_o.at[0, part], sem.at[2 + k])
        copy.start()
        copies.append(copy)
    for copy in copies:
        copy.wait()


def body(acts, grads_out, weight_grad, old_in_factor, old_out_factor):
    rows, width = weight_grad.shape[1:]
    hbm = pl.BlockSpec(memory_space=pltpu.HBM)
    vm = pl.BlockSpec(memory_space=pltpu.VMEM)
    dma = pltpu.SemaphoreType.DMA
    vmem = pltpu.VMEM
    packed = (CHIPS, ROWS, B)
    sent = (PEERS, ROWS, B)
    operands = [
        pltpu.with_memory_space_constraint(a, pltpu.HBM)
        for a in (acts, grads_out, weight_grad, old_in_factor, old_out_factor)
    ]
    nat, in_factor, out_factor, scale = pl.pallas_call(
        kernel,
        out_shape=(
            jax.ShapeDtypeStruct((rows, width), F32),
            jax.ShapeDtypeStruct((B, B), F32),
            jax.ShapeDtypeStruct((B, B), F32),
            jax.ShapeDtypeStruct((1, B), F32),
        ),
        in_specs=[hbm] * 5,
        out_specs=(vm,) * 4,
        scratch_shapes=[
            vmem(acts.shape[1:], BF16),
            vmem(acts.shape[1:], BF16),
            vmem((rows, width), BF16),
            vmem((B, B), F32),
            vmem((B, B), F32),
            vmem(packed, BF16),
            vmem(packed, BF16),
            vmem(packed, F32),
            vmem(packed, F32),
            vmem(packed, BF16),
            vmem(packed, BF16),
            vmem(sent, BF16),
            vmem(sent, BF16),
            vmem(sent, BF16),
            vmem(sent, BF16),
            vmem(packed, BF16),
            vmem(packed, BF16),
            vmem((rows, width), BF16),
            vmem((X * Y - 1, 1, B), F32),
            vmem((Z * CORE - 1, 1, B), F32),
            vmem((1, B), F32),
            vmem((1, B), F32),
            dma((5,)),
            dma((2, 2)),
            dma((2, 2)),
            dma((2,)),
            dma((2, 2)),
            dma,
            dma((PEERS,)),
            dma,
            dma((CHIPS,)),
            dma((2,)),
            dma((2,)),
        ],
        compiler_params=pltpu.CompilerParams(
            collective_id=1, has_side_effects=True, vmem_limit_bytes=24 * 1024 * 1024
        ),
        name="kfac",
    )(*operands)
    return pl.pallas_call(
        finish,
        out_shape=(
            jax.ShapeDtypeStruct((1, rows, width), BF16),
            jax.ShapeDtypeStruct(old_in_factor.shape, F32),
            jax.ShapeDtypeStruct(old_out_factor.shape, F32),
        ),
        in_specs=[vm] * 4,
        out_specs=(hbm,) * 3,
        scratch_shapes=[vmem((rows, width), BF16), dma((6,))],
        compiler_params=pltpu.CompilerParams(vmem_limit_bytes=8 * 1024 * 1024),
        name="finish",
    )(nat, scale, in_factor, out_factor)


def solution(mesh):
    torus = Mesh(
        mesh.devices.reshape(X, YL, Z, YH, CORE),
        ("section_0", "section_1", "dp_0", "dp_1", "dp_2"),
    )
    in_specs = (
        P(SECTION, None, DP, None),
        P(SECTION, None, DP, None),
        P(SECTION, DP, None),
        P(SECTION, DP, None, None),
        P(SECTION, DP, None, None),
    )
    out_specs = (P(SECTION, DP, None), P(SECTION, DP, None, None), P(SECTION, DP, None, None))
    return jax.shard_map(body, mesh=torus, in_specs=in_specs, out_specs=out_specs, check_vma=False)
```

```python
import jax
import jax.numpy as jnp
from jax import lax
from jax.experimental import pallas as pl
from jax.experimental.pallas import tpu as pltpu
from jax.sharding import Mesh
from jax.sharding import PartitionSpec as P

ITERS = 8
SECTION = ("section_0", "section_1")
DP = ("dp_0", "dp_1", "dp_2")
DECAY = 0.7
DAMPING = 0.1
CLIP = 0.04
HIGH = lax.Precision.HIGHEST
LOGICAL = pl.DeviceIdType.LOGICAL

X, YL, Z, YH, CORE = 4, 4, 8, 2, 2
Y = YH * YL
CHIPS = Z * YH
PEERS = CHIPS - 1
B = 128
H = B // 2
ROWS = H + 8
SENT = H + 2
GROUP = 5
F32 = jnp.float32
BF16 = jnp.bfloat16


def iotas():
    return (
        lax.broadcasted_iota(jnp.int32, (H, B), 0),
        lax.broadcasted_iota(jnp.int32, (H, B), 1),
    )


def pack(full):
    r, l = iotas()
    top, low = full[:H], pltpu.roll(full[H:], H, 1)
    body = jnp.where((l < H) & (r > l), low, top)
    diag = jnp.sum(jnp.where(r == l, low, 0.0), axis=0, keepdims=True)
    return body, jnp.broadcast_to(diag, (ROWS - H, B))


def unpack(packed):
    r, l = iotas()
    body, diag = packed[:H], packed[H : H + 1]
    turned = jnp.concatenate([body, jnp.zeros((H, B), F32)], axis=0).T
    left_t, right_t = turned[:H], turned[H:]
    top = jnp.where((l < H) & (r > l), left_t, body)
    corner = jnp.where(r > l, body, jnp.where(r == l, diag, left_t))
    bottom = jnp.where(l < H, right_t, pltpu.roll(corner, H, 1))
    return jnp.concatenate([top, bottom], axis=0)


def eye():
    return (
        lax.broadcasted_iota(jnp.int32, (B, B), 0) == lax.broadcasted_iota(jnp.int32, (B, B), 1)
    ).astype(F32)


def parts(a):
    high = a.astype(BF16)
    return high, (a - high.astype(F32)).astype(BF16)


def dot(a, b):
    (ah, al), (bh, bl) = parts(a), parts(b)
    left = jnp.concatenate([ah, ah, al], axis=1)
    right = jnp.concatenate([bh, bl, bh], axis=0)
    return jnp.dot(left, right, preferred_element_type=F32)


def newton(factor):
    one = eye()
    damped = factor + DAMPING * one
    inv = 1.0 / jnp.sqrt(jnp.sum(damped * damped, keepdims=True))
    rest = one - inv * damped
    approx = inv * (one + rest)
    rest = dot(rest, rest)
    for _ in range(ITERS - 2):
        both = dot(rest, jnp.concatenate([rest, approx], axis=1))
        approx = approx + both[:, B:]
        rest = both[:, :B]
    return approx + dot(rest, approx)


def offset(i):
    j = i % Z
    return 4 + ((j + 1) // 2) * (1 - 2 * (j % 2)), 1 - i // Z


def kernel(
    acts, grads, wgrad, old_in, old_out,
    nat, fi, fo, scale_o,
    tok_in, tok_out, wv, oi, oo,
    pk_in, pk_out, own_in, own_out, d2d_in, d2d_out,
    comb_in, comb_out, rx_in, rx_out,
    xd, xf, left, q1, q2, mine, mine2,
    ld, d_s, d_r, a_s, a_r, g_s, g_r, f_s, f_r, q_s, q_r,
):
    x, yl = lax.axis_index("section_0"), lax.axis_index("section_1")
    z, yh, c = lax.axis_index("dp_0"), lax.axis_index("dp_1"), lax.axis_index("dp_2")
    y = yh * YL + yl

    z_ahead = [lax.rem(z + d, Z) for d in range(Z)]
    y_ahead = [lax.rem(y + d, Y) for d in range(Y)]
    x_at = [lax.rem(x + d, X) * (YL * Z * YH * CORE) for d in range(X)]
    y_at = [lax.rem(t, YL) * (Z * YH * CORE) + lax.div(t, YL) * CORE for t in y_ahead]
    z_at = [t * (YH * CORE) for t in z_ahead]
    c_at = [c, 1 - c]

    def device(dx=0, dy=0, dz=0, dc=0):
        return x_at[dx] + y_at[dy] + z_at[dz] + c_at[dc]

    partner = device(dc=1)
    chips = [device(dy=YL * offset(i)[1], dz=offset(i)[0]) for i in range(PEERS)]
    plane = [(dx, dy) for dx in (2, 1, 3, 0) for dy in (4, 3, 5, 2, 6, 1, 7, 0)][:-1]
    column = [(dz, dc) for dz in (4, 3, 5, 2, 6, 1, 7, 0) for dc in (1, 0)][:-1]
    planes = [device(dx=dx, dy=dy) for dx, dy in plane]
    columns = [device(dz=dz, dc=dc) for dz, dc in column]
    greeted = (
        chips
        + [partner]
        + [d for d, at in zip(planes, plane, strict=True) if at != (0, YL)]
        + [d for d, at in zip(columns, column, strict=True) if at[0] and at[1]]
    )
    barrier = pltpu.get_barrier_semaphore()
    for target in greeted[:PEERS]:
        pl.semaphore_signal(barrier, inc=1, device_id=target, device_id_type=LOGICAL)
    loads = [
        pltpu.make_async_copy(acts.at[0], tok_in, ld.at[0]),
        pltpu.make_async_copy(grads.at[0], tok_out, ld.at[1]),
        pltpu.make_async_copy(old_in.at[0, 0], oi, ld.at[2]),
        pltpu.make_async_copy(old_out.at[0, 0], oo, ld.at[3]),
        pltpu.make_async_copy(wgrad.at[0], wv, ld.at[4]),
    ]
    for copy in loads:
        copy.start()
    for target in greeted[PEERS:]:
        pl.semaphore_signal(barrier, inc=1, device_id=target, device_id_type=LOGICAL)

    def chip_to(i):
        dz, dy = offset(i)
        return lax.rem(z + dz, Z) * YH + lax.rem(yh + dy, YH)

    def chip_from(i):
        dz, dy = offset(i)
        return lax.rem(z + Z - dz, Z) * YH + lax.rem(yh + dy, YH)

    def columns_of(chip, core):
        return pl.ds(pl.multiple_of((chip * CORE + core) * B, B), B)

    def grams(tok, core, out):
        @pl.loop(0, CHIPS // 4)
        def _(g):
            for u in range(4):
                i = g * 4 + u
                t = tok[:, :, columns_of(chip_to(i), core)].reshape(B, B)
                full = lax.dot_general(
                    t, t, (((0,), (0,)), ((), ())), preferred_element_type=F32
                )
                body, diag = pack(full)
                out[i, :H] = body.astype(out.dtype)
                out[i, H:] = diag.astype(out.dtype)

    def remote(src, dst, send, recv, target):
        return pltpu.make_async_remote_copy(
            src_ref=src, dst_ref=dst, send_sem=send, recv_sem=recv,
            device_id=target, device_id_type=LOGICAL,
        )

    def sent(ref, at):
        return ref.at[at, pl.ds(0, SENT)]

    def combine(kind, own, got, comb, rx, these):
        for i in these:
            comb[i] = (own[i] + got[i].astype(F32)).astype(BF16)
            landed = a_r.at[kind, i // Z]
            remote(sent(comb, i), sent(rx, i), a_s.at[kind], landed, chips[i]).start()

    def whole(ref, sem):
        return pltpu.make_async_copy(ref, ref, sem)

    def collect(kind, side, rx, acc):
        these = (range(Z), range(Z, PEERS))[side]
        whole(sent(rx, pl.ds(these[0], len(these))), a_r.at[kind, side]).wait()
        for i in these:
            acc = acc + rx[i].astype(F32)
        return acc

    def mine_of(own, got):
        return own[PEERS] + got[PEERS].astype(F32)

    def halves(kind, src, dst):
        return [
            remote(sent(src, half), sent(dst, half), d_s.at[kind, h], d_r.at[kind, h], partner)
            for h, half in enumerate((pl.ds(0, Z), pl.ds(Z, Z)))
        ]

    count = F32(4.0 * 32 * Z * YH * CORE)

    loads[0].wait()
    grams(tok_in, 1 - c, pk_in)
    grams(tok_in, c, own_in)
    pl.semaphore_wait(barrier, len(greeted))
    in_pair = halves(0, pk_in, d2d_in)
    for half in in_pair:
        half.start()
    loads[1].wait()
    grams(tok_out, 1 - c, pk_out)
    out_pair = halves(1, pk_out, d2d_out)
    for half in out_pair:
        half.start()
    in_pair[0].wait_recv()
    combine(0, own_in, d2d_in, comb_in, rx_in, range(Z))
    in_pair[1].wait_recv()
    combine(0, own_in, d2d_in, comb_in, rx_in, range(Z, PEERS))
    grams(tok_out, c, own_out)
    for half in out_pair:
        half.wait_recv()
    for copy in loads[2:]:
        copy.wait()
    combine(1, own_out, d2d_out, comb_out, rx_out, range(Z))
    in_sum = collect(0, 1, rx_in, mine_of(own_in, d2d_in))
    combine(1, own_out, d2d_out, comb_out, rx_out, range(Z, PEERS))
    gram_in = unpack(collect(0, 0, rx_in, in_sum))
    in_factor = DECAY * oi[...] + ((1.0 - DECAY) / count) * gram_in
    fi[...] = in_factor
    body, diag = pack(newton(in_factor))
    xd[PEERS, :H] = body.astype(BF16)
    xd[PEERS, H:] = diag.astype(BF16)

    def gather(i):
        return remote(sent(xd, PEERS), sent(xd, i), g_s, g_r.at[i], partner)

    def forward(i):
        return remote(sent(xd, i), sent(xf, i), f_s, f_r.at[i], partner)

    for i in range(PEERS):
        remote(sent(xd, PEERS), sent(xd, i), g_s, g_r.at[i], chips[i]).start()
    forward(PEERS).start()

    out_sum = collect(1, 1, rx_out, mine_of(own_out, d2d_out))
    gram_out = unpack(collect(1, 0, rx_out, out_sum))
    out_factor = DECAY * oo[...] + ((1.0 - DECAY) / count) * gram_out
    fo[...] = out_factor
    out_inverse = newton(out_factor).astype(BF16)

    @pl.loop(0, 2)
    def _(k):
        for u in range(4):
            at = pl.ds(pl.multiple_of(k * 2048 + u * 512, 512), 512)
            left[:, at] = jnp.dot(out_inverse, wv[:, at], preferred_element_type=F32).astype(BF16)

    def block(packed, i, core, acc):
        inverse = unpack(packed[i].astype(F32)).astype(BF16)
        at = columns_of(chip_from(i), core)
        part = jnp.dot(left[:, at], inverse, preferred_element_type=F32)
        nat[:, at] = part
        part = part * wv[:, at].astype(F32)
        return acc + jnp.sum(part.reshape(B // 8, 8, B), axis=0)

    def arrived(g):
        these = [PEERS - 1 - g * GROUP - u for u in range(GROUP)]
        for i in these:
            gather(i).wait_recv()
            forward(i).start()
        return these

    def both(g, acc):
        these = arrived(g)
        for i in these:
            forward(i + GROUP).wait_recv()
        for i in these:
            acc = block(xd, i, c, acc)
            acc = block(xf, i + GROUP, 1 - c, acc)
        return acc

    acc = block(xd, PEERS, c, jnp.zeros((8, B), F32))
    for i in arrived(0):
        acc = block(xd, i, c, acc)
    forward(PEERS).wait_recv()
    acc = block(xf, PEERS, 1 - c, acc)
    acc = lax.fori_loop(1, PEERS // GROUP, both, acc)
    for i in range(GROUP):
        forward(i).wait_recv()
    for i in range(GROUP):
        acc = block(xf, i, 1 - c, acc)

    mine[...] = jnp.broadcast_to(jnp.sum(acc, keepdims=True), (1, B))
    for k, target in enumerate(planes):
        remote(mine, q1.at[k], q_s.at[0], q_r.at[0], target).start()
    whole(q1, q_r.at[0]).wait()
    quad = mine[...] + jnp.sum(q1[...], axis=0)
    mine2[...] = quad
    for k, target in enumerate(columns):
        remote(mine2, q2.at[k], q_s.at[1], q_r.at[1], target).start()
    whole(q2, q_r.at[1]).wait()
    quad = quad + jnp.sum(q2[...], axis=0)
    numel = F32(X * YL * 4096.0 * 4096.0)
    scale_o[...] = jnp.minimum(1.0, jnp.sqrt(CLIP * numel / quad))

    for half in in_pair + out_pair:
        half.wait_send()
    every = pl.ds(0, PEERS)
    whole(sent(comb_in, every), a_s.at[0]).wait()
    whole(sent(comb_out, every), a_s.at[1]).wait()
    whole(sent(rx_in, every), g_s).wait()
    whole(sent(xf, pl.ds(0, CHIPS)), f_s).wait()
    whole(q1, q_s.at[0]).wait()
    whole(q2, q_s.at[1]).wait()


def finish(nat, scale, in_factor, out_factor, update_o, in_o, out_o, up, sem):
    copies = [
        pltpu.make_async_copy(in_factor, in_o.at[0, 0], sem.at[0]),
        pltpu.make_async_copy(out_factor, out_o.at[0, 0], sem.at[1]),
    ]
    for copy in copies:
        copy.start()
    factor = scale[...]
    pieces, rows = 4, nat.shape[0] // 4
    for k in range(pieces):
        part = pl.ds(k * rows, rows)
        up[part] = (factor[:, :1] * nat[part]).astype(BF16)
        copy = pltpu.make_async_copy(up.at[part], update_o.at[0, part], sem.at[2 + k])
        copy.start()
        copies.append(copy)
    for copy in copies:
        copy.wait()


def body(acts, grads_out, weight_grad, old_in_factor, old_out_factor):
    rows, width = weight_grad.shape[1:]
    hbm = pl.BlockSpec(memory_space=pltpu.HBM)
    vm = pl.BlockSpec(memory_space=pltpu.VMEM)
    dma = pltpu.SemaphoreType.DMA
    vmem = pltpu.VMEM
    packed = (CHIPS, ROWS, B)
    sent = (PEERS, ROWS, B)
    operands = [
        pltpu.with_memory_space_constraint(a, pltpu.HBM)
        for a in (acts, grads_out, weight_grad, old_in_factor, old_out_factor)
    ]
    nat, in_factor, out_factor, scale = pl.pallas_call(
        kernel,
        out_shape=(
            jax.ShapeDtypeStruct((rows, width), F32),
            jax.ShapeDtypeStruct((B, B), F32),
            jax.ShapeDtypeStruct((B, B), F32),
            jax.ShapeDtypeStruct((1, B), F32),
        ),
        in_specs=[hbm] * 5,
        out_specs=(vm,) * 4,
        scratch_shapes=[
            vmem(acts.shape[1:], BF16),
            vmem(acts.shape[1:], BF16),
            vmem((rows, width), BF16),
            vmem((B, B), F32),
            vmem((B, B), F32),
            vmem(packed, BF16),
            vmem(packed, BF16),
            vmem(packed, F32),
            vmem(packed, F32),
            vmem(packed, BF16),
            vmem(packed, BF16),
            vmem(sent, BF16),
            vmem(sent, BF16),
            vmem(sent, BF16),
            vmem(sent, BF16),
            vmem(packed, BF16),
            vmem(packed, BF16),
            vmem((rows, width), BF16),
            vmem((X * Y - 1, 1, B), F32),
            vmem((Z * CORE - 1, 1, B), F32),
            vmem((1, B), F32),
            vmem((1, B), F32),
            dma((5,)),
            dma((2, 2)),
            dma((2, 2)),
            dma((2,)),
            dma((2, 2)),
            dma,
            dma((PEERS,)),
            dma,
            dma((CHIPS,)),
            dma((2,)),
            dma((2,)),
        ],
        compiler_params=pltpu.CompilerParams(
            collective_id=1, has_side_effects=True, vmem_limit_bytes=24 * 1024 * 1024
        ),
        name="kfac",
    )(*operands)
    return pl.pallas_call(
        finish,
        out_shape=(
            jax.ShapeDtypeStruct((1, rows, width), BF16),
            jax.ShapeDtypeStruct(old_in_factor.shape, F32),
            jax.ShapeDtypeStruct(old_out_factor.shape, F32),
        ),
        in_specs=[vm] * 4,
        out_specs=(hbm,) * 3,
        scratch_shapes=[vmem((rows, width), BF16), dma((6,))],
        compiler_params=pltpu.CompilerParams(vmem_limit_bytes=8 * 1024 * 1024),
        name="finish",
    )(nat, scale, in_factor, out_factor)


def solution(mesh):
    torus = Mesh(
        mesh.devices.reshape(X, YL, Z, YH, CORE),
        ("section_0", "section_1", "dp_0", "dp_1", "dp_2"),
    )
    in_specs = (
        P(SECTION, None, DP, None),
        P(SECTION, None, DP, None),
        P(SECTION, DP, None),
        P(SECTION, DP, None, None),
        P(SECTION, DP, None, None),
    )
    out_specs = (P(SECTION, DP, None), P(SECTION, DP, None, None), P(SECTION, DP, None, None))
    return jax.shard_map(body, mesh=torus, in_specs=in_specs, out_specs=out_specs, check_vma=False)
```
